32 devices in a mesh: tm: 16 (over z, x, core), gz: 2 (over y).
Axes of the slice: x: 2, y: 2, z: 4, core: 2. Of those that a mesh axis runs over, the one named last changes fastest.
Arguments:
- starts: float32 [16, 8, 32, 128], P('tm', 'gz'), may hold values from -6 to 6
- cell_rates: float32 [8, 32, 128], P('gz'), may hold values from 0.3 to 1
Outputs:
- slab_ends: float32 [16, 8, 32, 128], P('tm', 'gz')
- next_starts: float32 [16, 8, 32, 128], P('tm', 'gz')
The draws below stay inside these ranges and needn't reach their ends.
All inputs are finite; a program needn't handle non-finite values.
Results may differ from the reference program's by a relative error of at most 0.0001.
Values sent between devices are 32-bit elements; how exact they have to be, the bound alone decides.
A program may use at most 64 MiB of HBM per device.

```python
import jax
import jax.numpy as jnp
from jax import lax

NX = 32
NY = 128
FINE = 4
SLABS = 16
NZ = 8


def draw_starts(key, part):
    rough = jnp.clip(jax.random.normal(key, (SLABS, NZ, NX, NY), jnp.float32), -6.0, 6.0)
    return rough


def block_levels(own_key, extent, pieces, low, largest):
    def one(position, blocks):
        draws = jax.random.uniform(jax.random.fold_in(jax.random.fold_in(own_key, 6), position), (blocks,), jnp.float32, low / len(pieces), largest / len(pieces))
        return jnp.repeat(jnp.exp(draws), extent[position] // blocks).reshape((-1,) + (1,) * (len(extent) - position - 1))

    factor_of = one(*pieces[0])
    for cut in pieces[1:]:
        factor_of = factor_of * one(*cut)
    return factor_of


def setup_inputs(seed: int = 0) -> dict:
    keys = jax.random.split(jax.random.key(seed), 3)
    starts = draw_starts(jax.random.fold_in(keys[2], 71), 0)
    cell_rates = jnp.clip(0.3 + 0.7 * jax.random.uniform(keys[1], (NZ, NX, NY), jnp.float32) ** block_levels(keys[1], (NZ, NX, NY), ((0, 2),), -0.2, 0.2), 0.3, 1.0)
    return dict(starts=starts, cell_rates=cell_rates)


fine_along_z = (0.1, 0.12)
fine_along_x = (0.15, 0.12)
fine_along_y = (0.2, 0.12)
coarse_along_z = (0.2, 0.25)
coarse_along_x = (0.3, 0.25)
coarse_along_y = (0.4, 0.25)


def line_filter(behind, middle, beyond, courant, diffuse):
    return (diffuse + 0.5 * courant) * behind + (1.0 - 2.0 * diffuse) * middle + (diffuse - 0.5 * courant) * beyond


def smooth_step(values, weights, along_z, along_x, along_y):
    mixed = line_filter(jnp.roll(values, 1, 2), values, jnp.roll(values, -1, 2), along_y[0], along_y[1])
    mixed = line_filter(jnp.roll(mixed, 1, 1), mixed, jnp.roll(mixed, -1, 1), along_x[0], along_x[1])
    mixed = line_filter(jnp.roll(mixed, 1, 0), mixed, jnp.roll(mixed, -1, 0), along_z[0], along_z[1])
    return values + weights * (mixed - values)


def restrict(values):
    extent_z, extent_x, extent_y = values.shape
    blocks = values.reshape(extent_z // 2, 2, extent_x // 2, 2, extent_y // 2, 2)
    return jnp.mean(blocks, axis=(1, 3, 5))


def prolong(values):
    extent_z, extent_x, extent_y = values.shape
    spread = jnp.broadcast_to(values[:, None, :, None, :, None], (extent_z, 2, extent_x, 2, extent_y, 2))
    return spread.reshape(extent_z * 2, extent_x * 2, extent_y * 2)


def propagate(values, coarse_rates):
    coarse = smooth_step(restrict(values), coarse_rates, coarse_along_z, coarse_along_x, coarse_along_y)
    return prolong(coarse)


def fine_solve(values, cell_rates):
    for sweep_index in range(FINE):
        values = smooth_step(values, cell_rates, fine_along_z, fine_along_x, fine_along_y)
    return values


def reference(starts, cell_rates):
    coarse_rates = restrict(cell_rates)

    def slab_correction(start):
        return fine_solve(start, cell_rates) - propagate(start, coarse_rates)

    correction = lax.map(slab_correction, starts)

    def link(current, term):
        finish = propagate(current, coarse_rates) + term
        return finish, finish

    _, slab_ends = lax.scan(link, starts[0], correction)
    next_starts = jnp.concatenate([slab_ends[-1:], slab_ends[:-1]], axis=0)
    return slab_ends, next_starts
```

```python
import functools

import jax
import jax.numpy as jnp
from jax import lax
from jax.experimental import pallas as pl
from jax.experimental.pallas import tpu as pltpu
from jax.sharding import PartitionSpec as P

MESH = pl.DeviceIdType.MESH
FINE = 4

fine_along_z = (0.1, 0.12)
fine_along_x = (0.15, 0.12)
fine_along_y = (0.2, 0.12)
coarse_along_z = (0.2, 0.25)
coarse_along_x = (0.3, 0.25)
coarse_along_y = (0.4, 0.25)


def line_filter(behind, middle, beyond, along):
    courant, diffuse = along
    return (
        (diffuse + 0.5 * courant) * behind
        + (1.0 - 2.0 * diffuse) * middle
        + (diffuse - 0.5 * courant) * beyond
    )


def turned(values, by, dim):
    return pltpu.roll(values, by % values.shape[dim], dim)


def filtered(values, by, dim, along):
    return line_filter(turned(values, by, dim), values, turned(values, -by, dim), along)


def group_size(slabs):
    return next(q for q in range(1, slabs + 1) if slabs % q == 0 and q * q >= slabs)


def kernel(
    slabs, parts, starts_ref, rates_ref, end_ref, next_ref,
    state, rates, mixed, coarse_held, terms, sums, corr, corr_before,
    load_sem, z_send, z_recv, term_send, term_recv, sum_send, sum_recv, corr_send, corr_recv,
):
    depth, rows, lanes = rates_ref.shape
    layers = depth * parts
    size = group_size(slabs)
    groups = slabs // size
    coarse_layers, coarse_rows = layers // 2, rows // 2
    half = coarse_layers // 2
    me, part = lax.axis_index("tm"), lax.axis_index("gz")
    group, place = me // size, lax.rem(me, size)
    after, before = lax.rem(me + 1, slabs), lax.rem(me + slabs - 1, slabs)

    own = pl.ds(part * depth, depth)
    loads = [
        pltpu.make_async_copy(starts_ref.at[0], state.at[own], load_sem.at[0]),
        pltpu.make_async_copy(rates_ref, rates.at[own], load_sem.at[1]),
    ]
    for load in loads:
        load.start()

    def part_at(i):
        return {"tm": me, "gz": lax.rem(part + i, parts)}

    def place_at(i):
        return {"tm": group * size + lax.rem(place + i, size), "gz": part}

    def group_at(i):
        return {"tm": lax.rem(group + i, groups) * size + place, "gz": part}

    barrier = pltpu.get_barrier_semaphore()
    peers = (
        [part_at(i) for i in range(1, parts)]
        + [place_at(i) for i in range(1, size)]
        + [group_at(i) for i in range(1, groups)]
        + [{"tm": after, "gz": part}, {"tm": before, "gz": part}]
    )
    for peer in peers:
        pl.semaphore_signal(barrier, inc=1, device_id=peer, device_id_type=MESH)
    pl.semaphore_wait(barrier, len(peers))

    def remote(ref, send_sem, recv_sem, peer):
        return pltpu.make_async_remote_copy(
            src_ref=ref, dst_ref=ref, send_sem=send_sem, recv_sem=recv_sem,
            device_id=peer, device_id_type=MESH,
        )

    z_copies = []
    for which, ref in enumerate((state, rates)):
        loads[which].wait()
        for i in range(1, parts):
            copy = remote(ref.at[own], z_send.at[which, i], z_recv.at[which, i], part_at(i))
            copy.start()
            z_copies.append(copy)
    for copy in z_copies:
        copy.wait()

    even = lax.rem(lax.broadcasted_iota(jnp.int32, (coarse_rows, lanes), 1), 2) == 0

    def evens(ref, layer):
        return ref[layer, pl.ds(0, coarse_rows, stride=2), :]

    def odds(ref, layer):
        return ref[layer, pl.ds(1, coarse_rows, stride=2), :]

    def restricted(ref, layer):
        total = (evens(ref, layer) + odds(ref, layer)) + (evens(ref, layer + 1) + odds(ref, layer + 1))
        pair = total + jnp.where(even, turned(total, -1, 1), turned(total, 1, 1))
        return pair * 0.125

    weights = [restricted(rates, 2 * k) for k in range(coarse_layers)]
    stays = [1.0 - weight for weight in weights]

    def advance(coarse):
        plane = [
            filtered(filtered(c, 2, 1, coarse_along_y), 1, 0, coarse_along_x) for c in coarse
        ]
        return [
            weights[k]
            * line_filter(
                plane[k - 1], plane[k], plane[(k + 1) % coarse_layers], coarse_along_z
            )
            + stays[k] * coarse[k]
            for k in range(coarse_layers)
        ]

    def packed_into(ref, slot, coarse):
        for k in range(half):
            ref[slot, k] = jnp.where(even, coarse[k], coarse[k + half])

    def unpacked(ref, slot):
        first, second = [], []
        for k in range(half):
            both = ref[slot, k]
            first.append(jnp.where(even, both, turned(both, 1, 1)))
            second.append(jnp.where(even, turned(both, -1, 1), both))
        return first + second

    gate = jnp.where(me > 0, 1.0, 0.0)
    guess = [gate * c for c in advance([restricted(state, 2 * k) for k in range(coarse_layers)])]
    for k in range(coarse_layers):
        coarse_held[k] = guess[k]

    for _ in range(FINE):
        for k in range(layers):
            mixed[k] = filtered(filtered(state[k], 1, 1, fine_along_y), 1, 0, fine_along_x)
        for k in range(layers):
            deep = line_filter(mixed[(k - 1) % layers], mixed[k], mixed[(k + 1) % layers], fine_along_z)
            held = state[k]
            state[k] = held + rates[k] * (deep - held)

    term = [restricted(state, 2 * k) - guess[k] for k in range(coarse_layers)]
    packed_into(terms, place, term)
    copies = []
    for i in range(1, size):
        copy = remote(terms.at[place], term_send.at[i], term_recv.at[i], place_at(i))
        copy.start()
        copies.append(copy)

    shift = part * (depth // 2)
    sides = [pl.ds(0, coarse_rows, stride=2), pl.ds(1, coarse_rows, stride=2)]
    for k in range(depth):
        for side in sides:
            corr[k, side, :] = state[part * depth + k, side, :] - coarse_held[shift + k // 2]
    corr_copy = pltpu.make_async_remote_copy(
        src_ref=corr, dst_ref=corr_before, send_sem=corr_send.at[0], recv_sem=corr_recv.at[0],
        device_id={"tm": after, "gz": part}, device_id_type=MESH,
    )
    corr_copy.start()

    for copy in copies:
        copy.wait()
    run = unpacked(terms, 0)
    kept = [jnp.zeros_like(c) for c in run]
    for step in range(1, size):
        kept = [jnp.where(place == step, new, old) for new, old in zip(run, kept)]
        run = [c + t for c, t in zip(advance(run), unpacked(terms, step))]
    packed_into(sums, group, run)
    copies = []
    for i in range(1, groups):
        copy = remote(sums.at[group], sum_send.at[i], sum_recv.at[i], group_at(i))
        copy.start()
        copies.append(copy)
    corr_copy.wait()
    for copy in copies:
        copy.wait()

    turns = jnp.where(me == 0, groups, group)
    started = jnp.where(turns > 0, 1.0, 0.0)

    def pass_group(index, coarse):
        coarse = list(coarse)
        for _ in range(size):
            coarse = advance(coarse)
        return tuple(c + t for c, t in zip(coarse, unpacked(sums, index)))

    coarse = tuple(started * c for c in unpacked(sums, 0))
    coarse = lax.fori_loop(1, turns, pass_group, coarse)
    coarse = lax.fori_loop(0, place, lambda _, c: tuple(advance(list(c))), coarse)
    coarse = [c + t for c, t in zip(coarse, kept)]
    for k in range(coarse_layers):
        coarse_held[k] = coarse[k]
    for k in range(depth // 2):
        offset = coarse_held[shift + k] - restricted(corr_before, 2 * k)
        for layer in (2 * k, 2 * k + 1):
            for side in sides:
                next_ref[0, layer, side, :] = corr_before[layer, side, :] + offset
    finish = advance(coarse)
    for k in range(coarse_layers):
        coarse_held[k] = gate * finish[k]
    for k in range(depth):
        for side in sides:
            end_ref[0, k, side, :] = corr[k, side, :] + coarse_held[shift + k // 2]


def solution(mesh):
    slabs, parts = mesh.shape["tm"], mesh.shape["gz"]

    def per_device(starts, cell_rates):
        depth, rows, lanes = cell_rates.shape
        layers = depth * parts
        size = group_size(slabs)
        groups = slabs // size
        whole = (layers, rows, lanes)
        coarse = (layers // 2, rows // 2, lanes)
        packed = (layers // 4, rows // 2, lanes)
        vmem, dma = pltpu.VMEM, pltpu.SemaphoreType.DMA
        return pl.pallas_call(
            functools.partial(kernel, slabs, parts),
            out_shape=[jax.ShapeDtypeStruct(starts.shape, jnp.float32)] * 2,
            in_specs=[pl.BlockSpec(memory_space=pl.ANY)] * 2,
            out_specs=[pl.BlockSpec(memory_space=pltpu.VMEM)] * 2,
            scratch_shapes=[
                vmem(whole, jnp.float32),
                vmem(whole, jnp.float32),
                vmem(whole, jnp.float32),
                vmem(coarse, jnp.float32),
                vmem((size,) + packed, jnp.float32),
                vmem((groups,) + packed, jnp.float32),
                vmem((depth, rows, lanes), jnp.float32),
                vmem((depth, rows, lanes), jnp.float32),
                dma((2,)),
                dma((2, parts)),
                dma((2, parts)),
                dma((size,)),
                dma((size,)),
                dma((groups,)),
                dma((groups,)),
                dma((1,)),
                dma((1,)),
            ],
            compiler_params=pltpu.CompilerParams(collective_id=0, has_side_effects=True),
        )(starts, cell_rates)

    return jax.shard_map(
        per_device,
        mesh=mesh,
        in_specs=(P("tm", "gz", None, None), P("gz", None, None)),
        out_specs=(P("tm", "gz", None, None), P("tm", "gz", None, None)),
        check_vma=False,
    )
```

```python
import functools

import jax
import jax.numpy as jnp
from jax import lax
from jax.experimental import pallas as pl
from jax.experimental.pallas import tpu as pltpu
from jax.sharding import PartitionSpec as P

MESH = pl.DeviceIdType.MESH
FINE = 4

fine_along_z = (0.1, 0.12)
fine_along_x = (0.15, 0.12)
fine_along_y = (0.2, 0.12)
coarse_along_z = (0.2, 0.25)
coarse_along_x = (0.3, 0.25)
coarse_along_y = (0.4, 0.25)


def line_filter(behind, middle, beyond, along):
    courant, diffuse = along
    return (
        (diffuse + 0.5 * courant) * behind
        + (1.0 - 2.0 * diffuse) * middle
        + (diffuse - 0.5 * courant) * beyond
    )


def turned(values, by, dim):
    return pltpu.roll(values, by % values.shape[dim], dim)


def filtered(values, by, dim, along):
    return line_filter(turned(values, by, dim), values, turned(values, -by, dim), along)


def row_size(slabs):
    return next(q for q in range(1, slabs + 1) if slabs % q == 0 and q * q >= slabs)


def group_size(slabs):
    return 2 if slabs % 2 == 0 else 1


def pair_size(size, depth):
    return 2 if size % 2 == 0 and depth % 2 == 0 else 1


def kernel(
    slabs, parts, starts_ref, rates_ref, end_ref, next_ref,
    state, rates, mixed, terms, sums, corr, corr_before,
    load_sem, state_send, state_recv, rate_send, rate_recv, pass_send, pass_recv,
    term_send, term_recv, sum_send, sum_recv, corr_sem, hop_sem,
):
    depth, rows, lanes = rates_ref.shape
    layers = depth * parts
    size = group_size(slabs)
    groups = slabs // size
    pair = pair_size(size, depth)
    share = depth // pair
    coarse_layers, coarse_rows = layers // 2, rows // 2
    half = coarse_layers // 2
    me, part = lax.axis_index("tm"), lax.axis_index("gz")
    group, place = me // size, lax.rem(me, size)
    wide = row_size(slabs)
    lines = slabs // wide
    line, column = me // wide, lax.rem(me, wide)
    after = lax.rem(me + 1, slabs)

    own = pl.ds(0, depth)
    rate_load = pltpu.make_async_copy(rates_ref, rates.at[own], load_sem.at[1])
    state_load = pltpu.make_async_copy(starts_ref.at[0], state.at[own], load_sem.at[0])
    rate_load.start()
    state_load.start()

    def part_at(i):
        return {"tm": me, "gz": lax.rem(part + i, parts)}

    def place_at(i):
        return {"tm": group * size + lax.rem(place + i, size), "gz": part}

    def group_at(i):
        return {"tm": lax.rem(group + i, groups) * size + place, "gz": part}

    def signal(sem, peer):
        pl.semaphore_signal(sem, inc=1, device_id=peer, device_id_type=MESH)

    lower, upper = line > 0, line < lines - 1
    beside = jnp.where(lower, 1, 0) + jnp.where(upper, 1, 0)

    def signal_beside(sem):
        @pl.when(lower)
        def _():
            signal(sem, {"tm": me - wide, "gz": part})

        @pl.when(upper)
        def _():
            signal(sem, {"tm": me + wide, "gz": part})

    barrier = pltpu.get_barrier_semaphore()
    near = [part_at(i) for i in range(1, parts)] + [
        {"tm": line * wide + lax.rem(column + i, wide), "gz": part} for i in range(1, wide)
    ]
    for peer in near:
        signal(barrier, peer)
    signal_beside(barrier)
    pl.semaphore_wait(barrier, len(near) + beside)

    def remote(src, dst, send_sem, recv_sem, peer):
        return pltpu.make_async_remote_copy(
            src_ref=src, dst_ref=dst, send_sem=send_sem, recv_sem=recv_sem,
            device_id=peer, device_id_type=MESH,
        )

    def started(copy):
        copy.start()
        return copy

    mine = lax.rem(me, pair) * share
    partner = {"tm": me + 1 - 2 * lax.rem(me, pair), "gz": part}
    arrivals = [(parts - i) * depth for i in range(1, parts)]
    rate_load.wait()
    rate_copies = [
        started(remote(
            rates.at[pl.ds(mine, share)], rates.at[pl.ds(at + mine, share)],
            rate_send.at[i], rate_recv.at[i], part_at(i + 1),
        ))
        for i, at in enumerate(arrivals)
    ]
    state_load.wait()
    state_copies = [
        started(remote(
            state.at[own], state.at[pl.ds(at, depth)], state_send.at[i], state_recv.at[i], part_at(i + 1)
        ))
        for i, at in enumerate(arrivals)
    ]
    for turn in range(lines - 1):
        signal_beside(hop_sem.at[turn])
        pl.semaphore_wait(hop_sem.at[turn], beside)

    pass_copies = []
    for i, at in enumerate(arrivals):
        rate_copies[i].wait()
        if pair > 1:
            piece = rates.at[pl.ds(at + mine, share)]
            pass_copies.append(
                started(remote(piece, piece, pass_send.at[i], pass_recv.at[i], partner))
            )

    def spread(first, last):
        for k in range(first, last):
            mixed[k] = filtered(filtered(state[k], 1, 1, fine_along_y), 1, 0, fine_along_x)

    spread(0, depth)
    for copy in state_copies:
        copy.wait()
    spread(depth, layers)
    for copy in pass_copies:
        copy.wait()

    even = lax.rem(lax.broadcasted_iota(jnp.int32, (coarse_rows, lanes), 1), 2) == 0
    sides = [pl.ds(0, coarse_rows, stride=2), pl.ds(1, coarse_rows, stride=2)]

    def restricted(ref, layer):
        total = (ref[layer, sides[0], :] + ref[layer, sides[1], :]) + (
            ref[layer + 1, sides[0], :] + ref[layer + 1, sides[1], :]
        )
        pair_sum = total + jnp.where(even, turned(total, -1, 1), turned(total, 1, 1))
        return pair_sum * 0.125

    weights = [restricted(rates, 2 * k) for k in range(coarse_layers)]
    stays = [1.0 - weight for weight in weights]

    def advance(coarse):
        plane = [
            filtered(filtered(c, 2, 1, coarse_along_y), 1, 0, coarse_along_x) for c in coarse
        ]
        return [
            weights[k]
            * line_filter(
                plane[k - 1], plane[k], plane[(k + 1) % coarse_layers], coarse_along_z
            )
            + stays[k] * coarse[k]
            for k in range(coarse_layers)
        ]

    def packed_into(ref, slot, coarse):
        for k in range(half):
            ref[slot, k] = jnp.where(even, coarse[k], coarse[k + half])

    def unpacked(ref, slot):
        first, second = [], []
        for k in range(half):
            both = ref[slot, k]
            first.append(jnp.where(even, both, turned(both, 1, 1)))
            second.append(jnp.where(even, turned(both, -1, 1), both))
        return first + second

    gate = jnp.where(me > 0, 1.0, 0.0)
    guess = [gate * c for c in advance([restricted(state, 2 * k) for k in range(coarse_layers)])]

    for turn in range(FINE):
        if turn > 0:
            spread(0, layers)
        for k in range(layers):
            deep = line_filter(mixed[(k - 1) % layers], mixed[k], mixed[(k + 1) % layers], fine_along_z)
            held = state[k]
            state[k] = held + rates[k] * (deep - held)

    packed_into(terms, place, [restricted(state, 2 * k) - guess[k] for k in range(coarse_layers)])
    block = terms.at[place]
    copies = [
        started(remote(block, block, term_send.at[i - 1], term_recv.at[i - 1], place_at(i)))
        for i in range(1, size)
    ]
    for k in range(depth):
        for side in sides:
            corr[k, side, :] = state[k, side, :] - guess[k // 2]
    corr_copy = started(remote(corr, corr_before, corr_sem.at[0], corr_sem.at[1], {"tm": after, "gz": part}))

    for copy in copies:
        copy.wait()
    run = unpacked(terms, 0)
    kept = [jnp.zeros_like(c) for c in run]
    for step in range(1, size):
        kept = [jnp.where(place == step, new, old) for new, old in zip(run, kept)]
        run = [c + t for c, t in zip(advance(run), unpacked(terms, step))]
    packed_into(sums, group, run)
    block = sums.at[group]
    def sum_copy(i):
        return remote(block, block, sum_send.at[i - 1], sum_recv.at[i - 1], group_at(i))

    first = me == 0
    for i in reversed(range(1, groups)):
        @pl.when((group + i < groups) | ((group + i == groups) & (place == 0)))
        def _():
            sum_copy(i).start()

    corr_copy.wait()
    before_coarse = [restricted(corr_before, 2 * k) for k in range(depth // 2)]
    for i in range(1, groups):
        @pl.when((group >= i) | first)
        def _():
            sum_copy(i).wait_recv()

    turns = jnp.where(me == 0, groups, group)
    begun = jnp.where(turns > 0, 1.0, 0.0)

    def pass_group(index, coarse):
        coarse = list(coarse)
        for _ in range(size):
            coarse = advance(coarse)
        return tuple(c + t for c, t in zip(coarse, unpacked(sums, index)))

    coarse = tuple(begun * c for c in unpacked(sums, 0))
    coarse = lax.fori_loop(1, turns, pass_group, coarse)
    coarse = lax.fori_loop(0, place, lambda _, c: tuple(advance(list(c))), coarse)
    coarse = [c + t for c, t in zip(coarse, kept)]
    finish = [gate * c for c in advance(coarse)]
    for k in range(depth):
        offset = coarse[k // 2] - before_coarse[k // 2]
        for side in sides:
            next_ref[0, k, side, :] = corr_before[k, side, :] + offset
            end_ref[0, k, side, :] = corr[k, side, :] + finish[k // 2]
    for i in range(1, groups):
        @pl.when((group + i < groups) | ((group + i == groups) & (place == 0)))
        def _():
            sum_copy(i).wait_send()


def hand_out_kernel(end_ref, next_ref, end_out, next_out, sems):
    copies = [
        pltpu.make_async_copy(end_ref, end_out, sems.at[0]),
        pltpu.make_async_copy(next_ref, next_out, sems.at[1]),
    ]
    for copy in copies:
        copy.start()
    for copy in copies:
        copy.wait()


def hand_out(end, following):
    return pl.pallas_call(
        hand_out_kernel,
        out_shape=[jax.ShapeDtypeStruct(end.shape, end.dtype)] * 2,
        in_specs=[pl.BlockSpec(memory_space=pltpu.VMEM)] * 2,
        out_specs=[pl.BlockSpec(memory_space=pl.ANY)] * 2,
        scratch_shapes=[pltpu.SemaphoreType.DMA((2,))],
    )(*(pltpu.with_memory_space_constraint(x, pltpu.VMEM) for x in (end, following)))


def solution(mesh):
    slabs, parts = mesh.shape["tm"], mesh.shape["gz"]

    def per_device(starts, cell_rates):
        depth, rows, lanes = cell_rates.shape
        layers = depth * parts
        size = group_size(slabs)
        groups = slabs // size
        whole = (layers, rows, lanes)
        packed = (layers // 4, rows // 2, lanes)
        vmem, dma = pltpu.VMEM, pltpu.SemaphoreType.DMA
        ends = pl.pallas_call(
            functools.partial(kernel, slabs, parts),
            out_shape=[pltpu.VMEM(starts.shape, jnp.float32)] * 2,
            in_specs=[pl.BlockSpec(memory_space=pl.ANY)] * 2,
            out_specs=[pl.BlockSpec(memory_space=pltpu.VMEM)] * 2,
            scratch_shapes=[
                vmem(whole, jnp.float32),
                vmem(whole, jnp.float32),
                vmem(whole, jnp.float32),
                vmem((size,) + packed, jnp.float32),
                vmem((groups,) + packed, jnp.float32),
                vmem((depth, rows, lanes), jnp.float32),
                vmem((depth, rows, lanes), jnp.float32),
                dma((2,)),
            ]
            + [dma((max(parts - 1, 1),))] * 6
            + [dma((max(size - 1, 1),))] * 2
            + [dma((max(groups - 1, 1),))] * 2
            + [dma((2,)), pltpu.SemaphoreType.REGULAR((max(slabs // row_size(slabs) - 1, 1),))],
            compiler_params=pltpu.CompilerParams(collective_id=0, has_side_effects=True),
        )(starts, cell_rates)
        return hand_out(*ends)

    return jax.shard_map(
        per_device,
        mesh=mesh,
        in_specs=(P("tm", "gz", None, None), P("gz", None, None)),
        out_specs=(P("tm", "gz", None, None), P("tm", "gz", None, None)),
        check_vma=False,
    )
```

```python
import functools

import jax
import jax.numpy as jnp
from jax import lax
from jax.experimental import pallas as pl
from jax.experimental.pallas import tpu as pltpu
from jax.sharding import PartitionSpec as P

MESH = pl.DeviceIdType.MESH
FINE = 4

fine_along_z = (0.1, 0.12)
fine_along_x = (0.15, 0.12)
fine_along_y = (0.2, 0.12)
coarse_along_z = (0.2, 0.25)
coarse_along_x = (0.3, 0.25)
coarse_along_y = (0.4, 0.25)


def line_filter(behind, middle, beyond, along):
    courant, diffuse = along
    return (
        (diffuse + 0.5 * courant) * behind
        + (1.0 - 2.0 * diffuse) * middle
        + (diffuse - 0.5 * courant) * beyond
    )


def turned(values, by, dim):
    return pltpu.roll(values, by % values.shape[dim], dim)


def filtered(values, by, dim, along):
    return line_filter(turned(values, by, dim), values, turned(values, -by, dim), along)


def row_size(slabs):
    return next(q for q in range(1, slabs + 1) if slabs % q == 0 and q * q >= slabs)


def group_size(slabs):
    return 2 if slabs % 2 == 0 else 1


def rounds(lines):
    reaches, known = [], 1
    while known < lines:
        reaches.append(known)
        known *= 2
    return reaches


def pair_size(size, depth):
    return 2 if size % 2 == 0 and depth % 2 == 0 else 1


def kernel(
    slabs, parts, starts_ref, rates_ref, end_ref, next_ref,
    state, rates, mixed, terms, sums, corr, corr_before,
    load_sem, state_send, state_recv, rate_send, rate_recv, pass_send, pass_recv,
    term_send, term_recv, sum_send, sum_recv, corr_sem, hop_sem,
):
    depth, rows, lanes = rates_ref.shape
    layers = depth * parts
    size = group_size(slabs)
    groups = slabs // size
    pair = pair_size(size, depth)
    share = depth // pair
    coarse_layers, coarse_rows = layers // 2, rows // 2
    half = coarse_layers // 2
    me, part = lax.axis_index("tm"), lax.axis_index("gz")
    group, place = me // size, lax.rem(me, size)
    wide = row_size(slabs)
    lines = slabs // wide
    line, column = me // wide, lax.rem(me, wide)
    after = lax.rem(me + 1, slabs)

    own = pl.ds(0, depth)
    rate_load = pltpu.make_async_copy(rates_ref, rates.at[own], load_sem.at[1])
    state_load = pltpu.make_async_copy(starts_ref.at[0], state.at[own], load_sem.at[0])
    rate_load.start()
    state_load.start()

    def part_at(i):
        return {"tm": me, "gz": lax.rem(part + i, parts)}

    def place_at(i):
        return {"tm": group * size + lax.rem(place + i, size), "gz": part}

    def group_at(i):
        return {"tm": lax.rem(group + i, groups) * size + place, "gz": part}

    def signal(sem, peer):
        pl.semaphore_signal(sem, inc=1, device_id=peer, device_id_type=MESH)

    def signal_beside(sem, reach):
        for d in range(1, reach + 1):
            @pl.when(line >= d)
            def _():
                signal(sem, {"tm": me - d * wide, "gz": part})

            @pl.when(line + d < lines)
            def _():
                signal(sem, {"tm": me + d * wide, "gz": part})

    def beside(reach):
        return jnp.minimum(line, reach) + jnp.minimum(lines - 1 - line, reach)

    barrier = pltpu.get_barrier_semaphore()
    near = [part_at(i) for i in range(1, parts)] + [
        {"tm": line * wide + lax.rem(column + i, wide), "gz": part} for i in range(1, wide)
    ]
    for peer in near:
        signal(barrier, peer)
    signal_beside(barrier, 1)
    pl.semaphore_wait(barrier, len(near) + beside(1))

    def remote(src, dst, send_sem, recv_sem, peer):
        return pltpu.make_async_remote_copy(
            src_ref=src, dst_ref=dst, send_sem=send_sem, recv_sem=recv_sem,
            device_id=peer, device_id_type=MESH,
        )

    def started(copy):
        copy.start()
        return copy

    mine = lax.rem(me, pair) * share
    partner = {"tm": me + 1 - 2 * lax.rem(me, pair), "gz": part}
    arrivals = [(parts - i) * depth for i in range(1, parts)]
    rate_load.wait()
    rate_copies = [
        started(remote(
            rates.at[pl.ds(mine, share)], rates.at[pl.ds(at + mine, share)],
            rate_send.at[i], rate_recv.at[i], part_at(i + 1),
        ))
        for i, at in enumerate(arrivals)
    ]
    def spread(first, last):
        for k in range(first, last):
            mixed[k] = filtered(filtered(state[k], 1, 1, fine_along_y), 1, 0, fine_along_x)

    state_load.wait()
    spread(0, depth)
    state_copies = [
        started(remote(
            state.at[own], state.at[pl.ds(at, depth)], state_send.at[i], state_recv.at[i], part_at(i + 1)
        ))
        for i, at in enumerate(arrivals)
    ]
    reaches = rounds(lines)
    for turn, reach in enumerate(reaches):
        signal_beside(hop_sem.at[turn], reach)
        if turn < len(reaches) - 1:
            pl.semaphore_wait(hop_sem.at[turn], beside(reach))

    pass_copies = []
    for i, at in enumerate(arrivals):
        rate_copies[i].wait_recv()
        if pair > 1:
            piece = rates.at[pl.ds(at + mine, share)]
            pass_copies.append(
                started(remote(piece, piece, pass_send.at[i], pass_recv.at[i], partner))
            )
    for reach in reaches[-1:]:
        pl.semaphore_wait(hop_sem.at[len(reaches) - 1], beside(reach))
    for copy in state_copies:
        copy.wait()
    spread(depth, layers)
    for copy in pass_copies:
        copy.wait()
    for copy in rate_copies:
        copy.wait_send()

    even = lax.rem(lax.broadcasted_iota(jnp.int32, (coarse_rows, lanes), 1), 2) == 0
    sides = [pl.ds(0, coarse_rows, stride=2), pl.ds(1, coarse_rows, stride=2)]

    def restricted(ref, layer):
        total = (ref[layer, sides[0], :] + ref[layer, sides[1], :]) + (
            ref[layer + 1, sides[0], :] + ref[layer + 1, sides[1], :]
        )
        pair_sum = total + jnp.where(even, turned(total, -1, 1), turned(total, 1, 1))
        return pair_sum * 0.125

    weights = [restricted(rates, 2 * k) for k in range(coarse_layers)]
    stays = [1.0 - weight for weight in weights]

    def advance(coarse):
        plane = [
            filtered(filtered(c, 2, 1, coarse_along_y), 1, 0, coarse_along_x) for c in coarse
        ]
        return [
            weights[k]
            * line_filter(
                plane[k - 1], plane[k], plane[(k + 1) % coarse_layers], coarse_along_z
            )
            + stays[k] * coarse[k]
            for k in range(coarse_layers)
        ]

    def packed_into(ref, slot, coarse):
        for k in range(half):
            ref[slot, k] = jnp.where(even, coarse[k], coarse[k + half])

    def unpacked(ref, slot):
        first, second = [], []
        for k in range(half):
            both = ref[slot, k]
            first.append(jnp.where(even, both, turned(both, 1, 1)))
            second.append(jnp.where(even, turned(both, -1, 1), both))
        return first + second

    gate = jnp.where(me > 0, 1.0, 0.0)
    guess = [gate * c for c in advance([restricted(state, 2 * k) for k in range(coarse_layers)])]

    for turn in range(FINE):
        if turn > 0:
            spread(0, layers)
        for k in range(layers):
            deep = line_filter(mixed[(k - 1) % layers], mixed[k], mixed[(k + 1) % layers], fine_along_z)
            held = state[k]
            state[k] = held + rates[k] * (deep - held)

    packed_into(terms, place, [restricted(state, 2 * k) - guess[k] for k in range(coarse_layers)])
    block = terms.at[place]
    copies = [
        started(remote(block, block, term_send.at[i - 1], term_recv.at[i - 1], place_at(i)))
        for i in range(1, size)
    ]
    for k in range(depth):
        for side in sides:
            corr[k, side, :] = state[k, side, :] - guess[k // 2]
    corr_copy = started(remote(corr, corr_before, corr_sem.at[0], corr_sem.at[1], {"tm": after, "gz": part}))

    for copy in copies:
        copy.wait()
    run = unpacked(terms, 0)
    kept = [jnp.zeros_like(c) for c in run]
    for step in range(1, size):
        kept = [jnp.where(place == step, new, old) for new, old in zip(run, kept)]
        run = [c + t for c, t in zip(advance(run), unpacked(terms, step))]
    packed_into(sums, group, run)
    block = sums.at[group]
    def sum_copy(i):
        return remote(block, block, sum_send.at[i - 1], sum_recv.at[i - 1], group_at(i))

    for i in reversed(range(1, groups)):
        @pl.when((group + i < groups) | ((group + i == groups) & (place == 0)))
        def _():
            sum_copy(i).start()

    turns = jnp.where(me == 0, groups, group)
    begun = jnp.where(turns > 0, 1.0, 0.0)

    def take(index):
        i = lax.rem(group - index + groups, groups) - 1
        held = sums.at[index]
        remote(held, held, sum_send.at[i], sum_recv.at[i], group_at(1)).wait_recv()

    def pass_group(index, coarse):
        take(index)
        coarse = list(coarse)
        for _ in range(size):
            coarse = advance(coarse)
        return tuple(c + t for c, t in zip(coarse, unpacked(sums, index)))

    @pl.when(group > 0)
    def _():
        take(0)

    coarse = tuple(begun * c for c in unpacked(sums, 0))
    coarse = lax.fori_loop(1, turns, pass_group, coarse)
    coarse = lax.fori_loop(0, place, lambda _, c: tuple(advance(list(c))), coarse)
    coarse = [c + t for c, t in zip(coarse, kept)]
    corr_copy.wait()
    before_coarse = [restricted(corr_before, 2 * k) for k in range(depth // 2)]
    finish = [gate * c for c in advance(coarse)]
    for k in range(depth):
        offset = coarse[k // 2] - before_coarse[k // 2]
        for side in sides:
            next_ref[0, k, side, :] = corr_before[k, side, :] + offset
            end_ref[0, k, side, :] = corr[k, side, :] + finish[k // 2]
    for i in range(1, groups):
        @pl.when((group + i < groups) | ((group + i == groups) & (place == 0)))
        def _():
            sum_copy(i).wait_send()


def hand_out_kernel(end_ref, next_ref, end_out, next_out, sems):
    copies = [
        pltpu.make_async_copy(end_ref, end_out, sems.at[0]),
        pltpu.make_async_copy(next_ref, next_out, sems.at[1]),
    ]
    for copy in copies:
        copy.start()
    for copy in copies:
        copy.wait()


def hand_out(end, following):
    return pl.pallas_call(
        hand_out_kernel,
        out_shape=[jax.ShapeDtypeStruct(end.shape, end.dtype)] * 2,
        in_specs=[pl.BlockSpec(memory_space=pltpu.VMEM)] * 2,
        out_specs=[pl.BlockSpec(memory_space=pl.ANY)] * 2,
        scratch_shapes=[pltpu.SemaphoreType.DMA((2,))],
    )(*(pltpu.with_memory_space_constraint(x, pltpu.VMEM) for x in (end, following)))


def solution(mesh):
    slabs, parts = mesh.shape["tm"], mesh.shape["gz"]

    def per_device(starts, cell_rates):
        depth, rows, lanes = cell_rates.shape
        layers = depth * parts
        size = group_size(slabs)
        groups = slabs // size
        whole = (layers, rows, lanes)
        packed = (layers // 4, rows // 2, lanes)
        vmem, dma = pltpu.VMEM, pltpu.SemaphoreType.DMA
        ends = pl.pallas_call(
            functools.partial(kernel, slabs, parts),
            out_shape=[pltpu.VMEM(starts.shape, jnp.float32)] * 2,
            in_specs=[pl.BlockSpec(memory_space=pl.ANY)] * 2,
            out_specs=[pl.BlockSpec(memory_space=pltpu.VMEM)] * 2,
            scratch_shapes=[
                vmem(whole, jnp.float32),
                vmem(whole, jnp.float32),
                vmem(whole, jnp.float32),
                vmem((size,) + packed, jnp.float32),
                vmem((groups,) + packed, jnp.float32),
                vmem((depth, rows, lanes), jnp.float32),
                vmem((depth, rows, lanes), jnp.float32),
                dma((2,)),
            ]
            + [dma((max(parts - 1, 1),))] * 6
            + [dma((max(size - 1, 1),))] * 2
            + [dma((max(groups - 1, 1),))] * 2
            + [dma((2,)), pltpu.SemaphoreType.REGULAR((max(len(rounds(slabs // row_size(slabs))), 1),))],
            compiler_params=pltpu.CompilerParams(collective_id=0, has_side_effects=True),
        )(starts, cell_rates)
        return hand_out(*ends)

    return jax.shard_map(
        per_device,
        mesh=mesh,
        in_specs=(P("tm", "gz", None, None), P("gz", None, None)),
        out_specs=(P("tm", "gz", None, None), P("tm", "gz", None, None)),
        check_vma=False,
    )
```

```python
import functools

import jax
import jax.numpy as jnp
from jax import lax
from jax.experimental import pallas as pl
from jax.experimental.pallas import tpu as pltpu
from jax.sharding import PartitionSpec as P

MESH = pl.DeviceIdType.MESH
FINE = 4

fine_along_z = (0.1, 0.12)
fine_along_x = (0.15, 0.12)
fine_along_y = (0.2, 0.12)
coarse_along_z = (0.2, 0.25)
coarse_along_x = (0.3, 0.25)
coarse_along_y = (0.4, 0.25)


def line_filter(behind, middle, beyond, along):
    courant, diffuse = along
    return (
        (diffuse + 0.5 * courant) * behind
        + (1.0 - 2.0 * diffuse) * middle
        + (diffuse - 0.5 * courant) * beyond
    )


def turned(values, by, dim):
    return pltpu.roll(values, by % values.shape[dim], dim)


def filtered(values, by, dim, along):
    return line_filter(turned(values, by, dim), values, turned(values, -by, dim), along)


def row_size(slabs):
    return next(q for q in range(1, slabs + 1) if slabs % q == 0 and q * q >= slabs)


def group_size(slabs):
    return 2 if slabs % 2 == 0 else 1


def rounds(lines):
    reaches, known = [], 1
    while known < lines:
        reaches.append(known)
        known *= 2
    return reaches


def pair_size(size, depth):
    return 2 if size % 2 == 0 and depth % 2 == 0 else 1


def kernel(
    slabs, parts, starts_ref, rates_ref, end_ref, next_ref,
    state, rates, mixed, terms, sums, corr, corr_before,
    load_sem, state_send, state_recv, rate_send, rate_recv, pass_send, pass_recv,
    term_send, term_recv, sum_send, sum_recv, corr_sem, hop_sem,
):
    depth, rows, lanes = rates_ref.shape
    layers = depth * parts
    size = group_size(slabs)
    groups = slabs // size
    pair = pair_size(size, depth)
    share = depth // pair
    coarse_layers, coarse_rows = layers // 2, rows // 2
    half = coarse_layers // 2
    me, part = lax.axis_index("tm"), lax.axis_index("gz")
    group, place = me // size, lax.rem(me, size)
    wide = row_size(slabs)
    lines = slabs // wide
    line, column = me // wide, lax.rem(me, wide)
    after = lax.rem(me + 1, slabs)

    own = pl.ds(0, depth)
    rate_load = pltpu.make_async_copy(rates_ref, rates.at[own], load_sem.at[1])
    state_load = pltpu.make_async_copy(starts_ref.at[0], state.at[own], load_sem.at[0])
    rate_load.start()
    state_load.start()

    def part_at(i):
        return {"tm": me, "gz": lax.rem(part + i, parts)}

    def place_at(i):
        return {"tm": group * size + lax.rem(place + i, size), "gz": part}

    def group_at(i):
        return {"tm": lax.rem(group + i, groups) * size + place, "gz": part}

    def signal(sem, peer):
        pl.semaphore_signal(sem, inc=1, device_id=peer, device_id_type=MESH)

    def signal_beside(sem, reach):
        for d in range(1, reach + 1):
            @pl.when(line >= d)
            def _():
                signal(sem, {"tm": me - d * wide, "gz": part})

            @pl.when(line + d < lines)
            def _():
                signal(sem, {"tm": me + d * wide, "gz": part})

    def beside(reach):
        return jnp.minimum(line, reach) + jnp.minimum(lines - 1 - line, reach)

    barrier = pltpu.get_barrier_semaphore()
    near = [part_at(i) for i in range(1, parts)] + [
        {"tm": line * wide + lax.rem(column + i, wide), "gz": part} for i in range(1, wide)
    ]
    for peer in near:
        signal(barrier, peer)
    signal_beside(barrier, 1)
    pl.semaphore_wait(barrier, len(near) + beside(1))

    def remote(src, dst, send_sem, recv_sem, peer):
        return pltpu.make_async_remote_copy(
            src_ref=src, dst_ref=dst, send_sem=send_sem, recv_sem=recv_sem,
            device_id=peer, device_id_type=MESH,
        )

    def started(copy):
        copy.start()
        return copy

    mine = lax.rem(me, pair) * share
    partner = {"tm": me + 1 - 2 * lax.rem(me, pair), "gz": part}
    arrivals = [(parts - i) * depth for i in range(1, parts)]
    rate_load.wait()
    rate_copies = [
        started(remote(
            rates.at[pl.ds(mine, share)], rates.at[pl.ds(at + mine, share)],
            rate_send.at[i], rate_recv.at[i], part_at(i + 1),
        ))
        for i, at in enumerate(arrivals)
    ]
    def spread(first, last):
        for k in range(first, last):
            mixed[k] = filtered(filtered(state[k], 1, 1, fine_along_y), 1, 0, fine_along_x)

    state_load.wait()
    state_copies = [
        started(remote(
            state.at[own], state.at[pl.ds(at, depth)], state_send.at[i], state_recv.at[i], part_at(i + 1)
        ))
        for i, at in enumerate(arrivals)
    ]
    spread(0, depth)
    reaches = rounds(lines)
    for turn, reach in enumerate(reaches):
        signal_beside(hop_sem.at[turn], reach)
        if turn < len(reaches) - 1:
            pl.semaphore_wait(hop_sem.at[turn], beside(reach))

    pass_copies = []
    for i, at in enumerate(arrivals):
        rate_copies[i].wait_recv()
        if pair > 1:
            piece = rates.at[pl.ds(at + mine, share)]
            pass_copies.append(
                started(remote(piece, piece, pass_send.at[i], pass_recv.at[i], partner))
            )
    for reach in reaches[-1:]:
        pl.semaphore_wait(hop_sem.at[len(reaches) - 1], beside(reach))
    for copy in state_copies:
        copy.wait()
    spread(depth, layers)
    for copy in pass_copies:
        copy.wait()
    for copy in rate_copies:
        copy.wait_send()

    even = lax.rem(lax.broadcasted_iota(jnp.int32, (coarse_rows, lanes), 1), 2) == 0
    sides = [pl.ds(0, coarse_rows, stride=2), pl.ds(1, coarse_rows, stride=2)]

    def restricted(ref, layer):
        total = (ref[layer, sides[0], :] + ref[layer, sides[1], :]) + (
            ref[layer + 1, sides[0], :] + ref[layer + 1, sides[1], :]
        )
        pair_sum = total + jnp.where(even, turned(total, -1, 1), turned(total, 1, 1))
        return pair_sum * 0.125

    weights = [restricted(rates, 2 * k) for k in range(coarse_layers)]
    stays = [1.0 - weight for weight in weights]

    def advance(coarse):
        plane = [
            filtered(filtered(c, 2, 1, coarse_along_y), 1, 0, coarse_along_x) for c in coarse
        ]
        return [
            weights[k]
            * line_filter(
                plane[k - 1], plane[k], plane[(k + 1) % coarse_layers], coarse_along_z
            )
            + stays[k] * coarse[k]
            for k in range(coarse_layers)
        ]

    def packed_into(ref, slot, coarse):
        for k in range(half):
            ref[slot, k] = jnp.where(even, coarse[k], coarse[k + half])

    def unpacked(ref, slot):
        first, second = [], []
        for k in range(half):
            both = ref[slot, k]
            first.append(jnp.where(even, both, turned(both, 1, 1)))
            second.append(jnp.where(even, turned(both, -1, 1), both))
        return first + second

    gate = jnp.where(me > 0, 1.0, 0.0)
    guess = [gate * c for c in advance([restricted(state, 2 * k) for k in range(coarse_layers)])]

    for turn in range(FINE):
        if turn > 0:
            spread(0, layers)
        for k in range(layers):
            deep = line_filter(mixed[(k - 1) % layers], mixed[k], mixed[(k + 1) % layers], fine_along_z)
            held = state[k]
            state[k] = held + rates[k] * (deep - held)

    packed_into(terms, place, [restricted(state, 2 * k) - guess[k] for k in range(coarse_layers)])
    block = terms.at[place]
    copies = [
        started(remote(block, block, term_send.at[i - 1], term_recv.at[i - 1], place_at(i)))
        for i in range(1, size)
    ]
    for k in range(depth):
        for side in sides:
            corr[k, side, :] = state[k, side, :] - guess[k // 2]
    corr_copy = started(remote(corr, corr_before, corr_sem.at[0], corr_sem.at[1], {"tm": after, "gz": part}))

    for copy in copies:
        copy.wait()
    run = unpacked(terms, 0)
    kept = [jnp.zeros_like(c) for c in run]
    for step in range(1, size):
        kept = [jnp.where(place == step, new, old) for new, old in zip(run, kept)]
        run = [c + t for c, t in zip(advance(run), unpacked(terms, step))]
    packed_into(sums, group, run)
    block = sums.at[group]
    def sum_copy(i):
        return remote(block, block, sum_send.at[i - 1], sum_recv.at[i - 1], group_at(i))

    for i in reversed(range(1, groups)):
        @pl.when((group + i < groups) | ((group + i == groups) & (place == 0)))
        def _():
            sum_copy(i).start()

    turns = jnp.where(me == 0, groups, group)
    begun = jnp.where(turns > 0, 1.0, 0.0)

    def take(index):
        i = lax.rem(group - index + groups, groups) - 1
        held = sums.at[index]
        remote(held, held, sum_send.at[i], sum_recv.at[i], group_at(1)).wait_recv()

    def pass_group(index, coarse):
        take(index)
        coarse = list(coarse)
        for _ in range(size):
            coarse = advance(coarse)
        return tuple(c + t for c, t in zip(coarse, unpacked(sums, index)))

    @pl.when(group > 0)
    def _():
        take(0)

    coarse = tuple(begun * c for c in unpacked(sums, 0))
    coarse = lax.fori_loop(1, turns, pass_group, coarse)
    coarse = lax.fori_loop(0, place, lambda _, c: tuple(advance(list(c))), coarse)
    coarse = [c + t for c, t in zip(coarse, kept)]
    corr_copy.wait()
    before_coarse = [restricted(corr_before, 2 * k) for k in range(depth // 2)]
    finish = [gate * c for c in advance(coarse)]
    for k in range(depth):
        offset = coarse[k // 2] - before_coarse[k // 2]
        for side in sides:
            next_ref[0, k, side, :] = corr_before[k, side, :] + offset
            end_ref[0, k, side, :] = corr[k, side, :] + finish[k // 2]
    for i in range(1, groups):
        @pl.when((group + i < groups) | ((group + i == groups) & (place == 0)))
        def _():
            sum_copy(i).wait_send()


def hand_out_kernel(end_ref, next_ref, end_out, next_out, sems):
    copies = [
        pltpu.make_async_copy(end_ref, end_out, sems.at[0]),
        pltpu.make_async_copy(next_ref, next_out, sems.at[1]),
    ]
    for copy in copies:
        copy.start()
    for copy in copies:
        copy.wait()


def hand_out(end, following):
    return pl.pallas_call(
        hand_out_kernel,
        out_shape=[jax.ShapeDtypeStruct(end.shape, end.dtype)] * 2,
        in_specs=[pl.BlockSpec(memory_space=pltpu.VMEM)] * 2,
        out_specs=[pl.BlockSpec(memory_space=pl.ANY)] * 2,
        scratch_shapes=[pltpu.SemaphoreType.DMA((2,))],
    )(*(pltpu.with_memory_space_constraint(x, pltpu.VMEM) for x in (end, following)))


def solution(mesh):
    slabs, parts = mesh.shape["tm"], mesh.shape["gz"]

    def per_device(starts, cell_rates):
        depth, rows, lanes = cell_rates.shape
        layers = depth * parts
        size = group_size(slabs)
        groups = slabs // size
        whole = (layers, rows, lanes)
        packed = (layers // 4, rows // 2, lanes)
        vmem, dma = pltpu.VMEM, pltpu.SemaphoreType.DMA
        ends = pl.pallas_call(
            functools.partial(kernel, slabs, parts),
            out_shape=[pltpu.VMEM(starts.shape, jnp.float32)] * 2,
            in_specs=[pl.BlockSpec(memory_space=pl.ANY)] * 2,
            out_specs=[pl.BlockSpec(memory_space=pltpu.VMEM)] * 2,
            scratch_shapes=[
                vmem(whole, jnp.float32),
                vmem(whole, jnp.float32),
                vmem(whole, jnp.float32),
                vmem((size,) + packed, jnp.float32),
                vmem((groups,) + packed, jnp.float32),
                vmem((depth, rows, lanes), jnp.float32),
                vmem((depth, rows, lanes), jnp.float32),
                dma((2,)),
            ]
            + [dma((max(parts - 1, 1),))] * 6
            + [dma((max(size - 1, 1),))] * 2
            + [dma((max(groups - 1, 1),))] * 2
            + [dma((2,)), pltpu.SemaphoreType.REGULAR((max(len(rounds(slabs // row_size(slabs))), 1),))],
            compiler_params=pltpu.CompilerParams(collective_id=0, has_side_effects=True),
        )(starts, cell_rates)
        return hand_out(*ends)

    return jax.shard_map(
        per_device,
        mesh=mesh,
        in_specs=(P("tm", "gz", None, None), P("gz", None, None)),
        out_specs=(P("tm", "gz", None, None), P("tm", "gz", None, None)),
        check_vma=False,
    )
```
